128 devices in a mesh: dp: 4 (over z), vocab: 32 (over y, x, core).
Axes of the slice: x: 4, y: 4, z: 4, core: 2. Of those that a mesh axis runs over, the one named last changes fastest.
Arguments:
- hidden: bfloat16 [2048, 5120], P('dp', 'vocab')
- weight: bfloat16 [5120, 77824], P(None, 'vocab'), may hold values from -0.078125 to 0.078125
- targets: int32 [2048], P('dp'), may hold values from 0 to 77823
- old_logprob: float32 [2048], P('dp'), may hold values from -13 to -10.5
- ref_logprob: float32 [2048], P('dp'), may hold values from -13 to -10.5
- lengths: int32 [32], P('dp'), may hold values from 1 to 64
- rewards: int32 [32], P('dp'), may hold values from 0 to 4
- group_ids: int32 [32], P('dp'), may hold values from 0 to 3, as said below
Outputs:
- token_logprob: float32 [2048], P('dp')
- entropy: float32 [2048], P('dp')
- advantage: float32 [2048], P('dp')
- loss: float32 [], replicated
The draws below stay inside these ranges and needn't reach their ends.
Inputs may be any that keep to these rules, and one draw needn't show every extreme that they name: `group_ids`: each prompt number is named by exactly 8 rollouts.
All inputs are finite; a program needn't handle non-finite values.
Results may differ from the reference program's by a relative error of at most 0.0003.
Values may be sent and summed in bfloat16 or wider, within the bound.
No kernel may reach another device: no remote copies, remote signals or barrier semaphores. Data moves between devices by JAX's collectives and lax.ppermute only.
A program may use at most 128 MiB of HBM per device.

```python
import math
from functools import partial
import jax
import jax.numpy as jnp
import numpy as np
from jax import lax

D = 5120
SEQ = 64
GROUP = 8
VOCAB = 77824
TOK_DEV = 512
ROLLOUTS = 32
TOKENS = 2048
PROMPTS = 4


def draw_hidden(key, part):
    values = jax.random.normal(jax.random.fold_in(key, 11), (TOKENS, D), jnp.float32)
    return values.astype(jnp.bfloat16)


def draw_group_ids(key, part):
    order = jax.random.permutation(jax.random.fold_in(key, 21), ROLLOUTS)
    return (order // GROUP).astype(jnp.int32)


def touch_ends(entries, key, smallest, largest):
    longest = entries.shape.index(max(entries.shape))
    spots = []
    for shift in (0, 1):
        where = [jax.random.randint(jax.random.fold_in(key, axis), (), 0, length) for axis, length in enumerate(entries.shape)]
        where[longest] = (where[longest] + shift) % entries.shape[longest]
        spots.append(tuple(where))
    return entries.at[spots[0]].set(smallest).at[spots[1]].set(largest)


def block_levels(key, shape, shards, smallest, largest):
    loudness = 1.0
    for dim, blocks in shards:
        draws = jax.random.uniform(jax.random.fold_in(jax.random.fold_in(key, 6), dim), (blocks,), jnp.float32, smallest / len(shards), largest / len(shards))
        loudness = loudness * jnp.repeat(jnp.exp(draws), shape[dim] // blocks).reshape((-1,) + (1,) * (len(shape) - 1 - dim))
    return loudness


def skewed_wide(own_key, dims, amount, slope):
    weights = [min(1 << octave, amount + 1 - (1 << octave)) * (1 << 20) // math.isqrt((1 << octave) ** slope) + 1 for octave in range((amount + 1).bit_length()) if 1 << octave <= amount]
    scale = 1 + sum(weights) // (1 << 30)
    table = np.cumsum(np.array([max(1, weight // scale) for weight in weights]))
    lot = jax.random.randint(jax.random.fold_in(own_key, 1), dims, 0, int(table[len(weights) - 1]))
    start = jnp.left_shift(1, jnp.searchsorted(jnp.asarray(table, jnp.int32), lot, side="right").astype(jnp.int32))
    standing = start - 1 + jax.random.randint(jax.random.fold_in(own_key, 4), dims, 0, 1 << 30) % jnp.minimum(start, amount + 1 - start)
    return jax.random.permutation(jax.random.fold_in(own_key, 2), amount)[standing].astype(jnp.int32)


def scatter_about(own_key, extent, scale, most, shards=(), held_as=jnp.bfloat16):
    entries = jax.random.normal(own_key, extent, jnp.float32) * scale
    if len(shards) > 0:
        entries = block_levels(own_key, extent, shards, -0.22, 0.18) * entries
    return jnp.clip(entries, min=-most, max=most).astype(held_as)


def setup_inputs(seed: int = 0) -> dict:
    streams_of = jax.random.split(jax.random.key(seed), 9)
    return {
        "hidden": draw_hidden(jax.random.fold_in(streams_of[8], 71), 0),
        "weight": scatter_about(streams_of[1], (D, VOCAB), D ** -0.5, 0.078125, ((1, 32),)),
        "targets": touch_ends(skewed_wide(streams_of[2], (TOKENS,), VOCAB, 2), jax.random.fold_in(streams_of[2], 3), 0, VOCAB - 1).astype(jnp.int32),
        "old_logprob": jnp.clip(-13.0 + 2.5 * jax.random.uniform(streams_of[3], (TOKENS,), jnp.float32) ** block_levels(streams_of[3], (TOKENS,), ((0, 4),), -0.2, 0.2), -13.0, -10.5),
        "ref_logprob": jnp.clip(-13.0 + 2.5 * jax.random.uniform(streams_of[4], (TOKENS,), jnp.float32) ** block_levels(streams_of[4], (TOKENS,), ((0, 4),), -0.2, 0.2), -13.0, -10.5),
        "lengths": touch_ends(jax.random.randint(streams_of[5], (ROLLOUTS,), 1, SEQ + 1), jax.random.fold_in(streams_of[5], 1), 1, SEQ).astype(jnp.int32),
        "rewards": touch_ends(jax.random.randint(streams_of[6], (ROLLOUTS,), 0, 5), jax.random.fold_in(streams_of[6], 1), 0, 4).astype(jnp.int32),
        "group_ids": draw_group_ids(jax.random.fold_in(streams_of[8], 71), 0),
    }


def head_block(weight, args):
    rows, picks = args
    logits = jnp.dot(rows, weight, preferred_element_type=jnp.float32)
    top = lax.optimization_barrier(jnp.max(logits, axis=1))
    scaled = jnp.exp(logits - top[:, None])
    total = lax.optimization_barrier(jnp.sum(scaled, axis=1))
    moment = lax.optimization_barrier(jnp.sum(scaled * logits, axis=1))
    lse = top + jnp.log(total)
    picked = jnp.take_along_axis(logits, picks[:, None], axis=1)[:, 0]
    return (picked - lse, lse - moment / total)

def reference(hidden, weight, targets, old_logprob, ref_logprob, lengths, rewards, group_ids):
    blocks = hidden.reshape(TOKENS // TOK_DEV, TOK_DEV, D)
    picks = targets.reshape(TOKENS // TOK_DEV, TOK_DEV).astype(jnp.int32)
    token_logprob, entropy = lax.map(partial(head_block, weight), (blocks, picks))
    token_logprob = token_logprob.reshape(TOKENS)
    entropy = entropy.reshape(TOKENS)
    member = (group_ids[:, None] == jnp.arange(PROMPTS, dtype=jnp.int32)[None, :]).astype(jnp.float32)
    scores = rewards.astype(jnp.float32)
    sums = jnp.dot(scores, member, precision=lax.Precision.HIGHEST)
    squares = jnp.dot(scores * scores, member, precision=lax.Precision.HIGHEST)
    mean = sums / GROUP
    spread = jnp.sqrt(jnp.maximum(squares / GROUP - mean * mean, 0.0))
    mean_r = jnp.dot(member, mean, precision=lax.Precision.HIGHEST)
    spread_r = jnp.dot(member, spread, precision=lax.Precision.HIGHEST)
    advantage = jnp.repeat((scores - mean_r) / jnp.maximum(spread_r, 1.0), SEQ)
    position = jnp.arange(SEQ, dtype=jnp.int32)
    mask = (position[None, :] < lengths[:, None]).astype(jnp.float32).reshape(TOKENS)
    ratio = jnp.exp(jnp.clip(token_logprob - old_logprob, -20.0, 20.0))
    surrogate = -jnp.minimum(ratio * advantage, jnp.clip(ratio, 0.8, 1.2) * advantage)
    shift = jnp.clip(ref_logprob - token_logprob, -20.0, 20.0)
    divergence = jnp.exp(shift) - shift - 1.0
    numer = jnp.sum(mask * (surrogate + 0.04 * divergence - 0.01 * entropy))
    loss = numer / jnp.sum(mask)
    return (token_logprob, entropy, advantage, loss)
```

```python
import functools

import jax
import jax.numpy as jnp
from jax import lax
from jax.experimental import pallas as pl
from jax.experimental.pallas import tpu as pltpu
from jax.sharding import PartitionSpec as P

GROUP = 8
LANES = 128
SIDE = 4
STEPS = (0, -1, 1, 2)
F32 = jnp.float32


def device(y, x, core):
    return ((y % SIDE) * SIDE + x % SIDE) * 2 + core


def everyone():
    return [(v // (2 * SIDE), v // 2 % SIDE, v % 2) for v in range(2 * SIDE * SIDE)]


def send_on(value, phase, step):
    pairs = []
    for y, x, core in everyone():
        to = (y, x + step, core) if core == phase else (y + step, x, core)
        pairs.append((device(y, x, core), device(*to)))
    return lax.ppermute(value, "vocab", pairs)


def swap(value):
    pairs = [(device(y, x, core), device(y, x, 1 - core)) for y, x, core in everyone()]
    return lax.ppermute(value, "vocab", pairs)


def over_dp(value, mask):
    return lax.ppermute(value, "dp", [(v, v ^ mask) for v in range(lax.axis_size("dp"))])


def block_rows(second, partner, depth):
    v = lax.axis_index("vocab")
    core = (v & 1) ^ partner
    x, y = (v >> 1) & (SIDE - 1), v >> 3
    rows = []
    for first in STEPS:
        dx = jnp.where(core == 0, first, second)
        dy = jnp.where(core == 0, second, first)
        block = (((y + dy) & (SIDE - 1)) * SIDE + ((x + dx) & (SIDE - 1))) * 2 + core
        rows.append(pl.multiple_of(block * depth, 32))
    return rows


def column_tiles(width):
    return [(b, min(b + 512, width)) for b in range(0, width, 512)]


def load_kernel(lo, hi, *refs):
    w_ref, out, sems = refs[0], refs[-2], refs[-1]
    count = sems.shape[0]
    size = (hi - lo) // count
    copies = [
        pltpu.make_async_copy(
            w_ref.at[pl.ds(lo + k * size, size)], out.at[pl.ds(lo + k * size, size)], sems.at[k]
        )
        for k in range(count)
    ]
    for c in copies:
        c.start()
    for c in copies:
        c.wait()


def multiply(parts, depth, refs, acc_in, acc, lhs):
    w_ref = refs[-1]
    rows, at = [], 0
    for ref, part in zip(refs, parts):
        size = ref.shape[0]
        lhs[:, at : at + size] = ref[...].T
        rows += block_rows(*part, depth)
        at += size
    for b, e in column_tiles(w_ref.shape[1]):
        w = jnp.concatenate([w_ref[pl.ds(r, depth), b:e] for r in rows], axis=0)
        out = jnp.dot(lhs[...], w, preferred_element_type=F32)
        acc[:, b:e] = out if acc_in is None else acc_in[:, b:e] + out


def first_kernel(parts, depth, *refs):
    acc, _, lhs = refs[len(parts) + 1 :]
    multiply(parts, depth, refs[: len(parts) + 1], None, acc, lhs)


def middle_kernel(parts, depth, *refs):
    acc_in, acc, _, lhs = refs[len(parts) + 1 :]
    multiply(parts, depth, refs[: len(parts) + 1], acc_in, acc, lhs)


def last_kernel(parts, depth, *refs):
    acc_in, target, stats, acc, lhs = refs[len(parts) + 1 :]
    multiply(parts, depth, refs[: len(parts) + 1], acc_in, acc, lhs)
    tok, width = acc.shape
    step = 64
    tops, totals, moments, picks = [], [], [], []
    lane = lax.broadcasted_iota(jnp.int32, (step, LANES), 1) + lax.axis_index("vocab") * width
    for r in range(0, tok, step):
        want = target[r : r + step, :] - lane
        top = acc[r : r + step, 0:LANES]
        pick = jnp.where(want == 0, top, 0.0)
        for b in range(LANES, width, LANES):
            piece = acc[r : r + step, b : b + LANES]
            top = jnp.maximum(top, piece)
            pick = jnp.where(want == b, piece, pick)
        total = jnp.zeros_like(top)
        moment = jnp.zeros_like(top)
        for b in range(0, width, LANES):
            piece = acc[r : r + step, b : b + LANES]
            scaled = jnp.exp(piece - top)
            total += scaled
            moment += scaled * piece
        tops.append(top)
        totals.append(total)
        moments.append(moment)
        picks.append(pick)
    top, total, moment, pick = (
        jnp.concatenate(p, axis=0).T for p in (tops, totals, moments, picks)
    )
    best = jnp.max(top, axis=0, keepdims=True)
    scale = jnp.exp(top - best)
    stats[0:1, :] = best
    stats[1:2, :] = jnp.sum(total * scale, axis=0, keepdims=True)
    stats[2:3, :] = jnp.sum(moment * scale, axis=0, keepdims=True)
    stats[3:4, :] = jnp.sum(pick, axis=0, keepdims=True)


def in_vmem(value):
    return pltpu.with_memory_space_constraint(value, pltpu.VMEM)


def vmem_specs(count):
    return [pl.BlockSpec(memory_space=pltpu.VMEM)] * count


def load(weight, held, lo, hi, pieces):
    weight_there = pltpu.with_memory_space_constraint(weight, pltpu.HBM)
    operands = (weight_there,) if held is None else (weight_there, in_vmem(held))
    return pl.pallas_call(
        functools.partial(load_kernel, lo, hi),
        out_shape=pltpu.VMEM(weight.shape, weight.dtype),
        in_specs=[pl.BlockSpec(memory_space=pltpu.HBM), *vmem_specs(len(operands) - 1)],
        out_specs=pl.BlockSpec(memory_space=pltpu.VMEM),
        scratch_shapes=[pltpu.SemaphoreType.DMA((pieces,))],
        input_output_aliases={} if held is None else {1: 0},
        cost_estimate=pl.CostEstimate(flops=1 << 31, bytes_accessed=1 << 20, transcendentals=0),
        compiler_params=pltpu.CompilerParams(vmem_limit_bytes=16 << 20),
    )(*operands)


def matmul(kernel, blocks, parts, rest, weight, out_shape, extra=()):
    depth_sum = sum(b.shape[0] for b in blocks)
    rows, width = blocks[0].shape[1], weight.shape[1]
    depth = weight.shape[0] // lax.axis_size("vocab")
    operands = (*blocks, weight, *rest)
    aliases = {}
    if kernel is not last_kernel:
        out_shape = (out_shape, jax.ShapeDtypeStruct(weight.shape, weight.dtype))
        aliases = {len(blocks): 1} | ({len(blocks) + 1: 0} if rest else {})
    return pl.pallas_call(
        functools.partial(kernel, parts, depth),
        out_shape=out_shape,
        in_specs=vmem_specs(len(operands)),
        out_specs=jax.tree.map(lambda _: pl.BlockSpec(memory_space=pltpu.VMEM), out_shape),
        scratch_shapes=[*extra, pltpu.VMEM((rows, depth_sum), jnp.bfloat16)],
        input_output_aliases=aliases,
        cost_estimate=pl.CostEstimate(
            flops=2 * rows * depth_sum * width, bytes_accessed=1 << 20, transcendentals=0
        ),
        compiler_params=pltpu.CompilerParams(vmem_limit_bytes=16 << 20),
    )(*[in_vmem(o) for o in operands])


def merged(stats, groups):
    size = len(groups[0])
    lines = lax.all_to_all(
        jnp.broadcast_to(stats[None], (size, *stats.shape)),
        "vocab", 0, 0, axis_index_groups=groups, tiled=True,
    )
    top = jnp.max(lines[:, 0], axis=0)
    scale = jnp.exp(lines[:, 0] - top[None])
    return jnp.stack(
        [
            top,
            jnp.sum(lines[:, 1] * scale, axis=0),
            jnp.sum(lines[:, 2] * scale, axis=0),
            jnp.sum(lines[:, 3], axis=0),
        ]
    )


def per_device(hidden, weight, targets, old_logprob, ref_logprob, lengths, rewards, group_ids):
    width = weight.shape[1]
    tok_rows = hidden.shape[0]
    acc_shape = jax.ShapeDtypeStruct((tok_rows, width), F32)
    features = hidden.T
    line = [features]
    for step in (1, -1, 2):
        line.append(send_on(features, 0, step))
    held = load(weight, None, 0, 3072, 4)
    held = load(weight, held, 3072, 5120, 4)
    line = jnp.concatenate(line, axis=0)
    far = []
    for step in (1, -1, 2):
        far.append(send_on(line, 1, step))
    line_p = swap(line)
    acc, held = matmul(first_kernel, (line, line_p), ((0, 0), (0, 1)), (), held, acc_shape)
    far_p = []
    for k in range(3):
        far_p.append(swap(far[k]))
    acc, held = matmul(middle_kernel, far[:2], ((-1, 0), (1, 0)), (acc,), held, acc_shape)
    acc, held = matmul(middle_kernel, far_p[:2], ((-1, 1), (1, 1)), (acc,), held, acc_shape)
    acc, held = matmul(middle_kernel, far[2:], ((2, 0),), (acc,), held, acc_shape)
    wanted_column = jnp.broadcast_to(targets[:, None], (tok_rows, LANES))
    stats = matmul(
        last_kernel, far_p[2:], ((2, 1),), (acc, wanted_column), held,
        jax.ShapeDtypeStruct((4, tok_rows), F32),
        extra=(pltpu.VMEM((tok_rows, width), F32),),
    )
    roll_rows = rewards.shape[0]
    prompt_count = roll_rows * lax.axis_size("dp") // GROUP
    member = (
        group_ids[:, None] == jnp.arange(prompt_count, dtype=jnp.int32)[None, :]
    ).astype(F32)
    scores = rewards.astype(F32)
    seq_len = tok_rows // roll_rows
    token = lax.broadcasted_iota(jnp.int32, (roll_rows, tok_rows), 1)
    own = token // seq_len == lax.broadcasted_iota(jnp.int32, (roll_rows, tok_rows), 0)
    live = own & (token % seq_len < lengths[:, None])
    mask = jnp.sum(live.astype(F32), axis=0)
    sums = jnp.concatenate(
        [
            jnp.sum(scores[:, None] * member, axis=0),
            jnp.sum((scores * scores)[:, None] * member, axis=0),
            jnp.sum(mask)[None],
            jnp.zeros((LANES - 2 * prompt_count - 1,), F32),
        ]
    )[None]
    sums = sums + over_dp(sums, 1)
    sums = sums + over_dp(sums, 3)

    rows = [[device(y, x, c) for x in range(SIDE) for c in range(2)] for y in range(SIDE)]
    columns = [[device(y, x, c) for y in range(SIDE)] for x in range(SIDE) for c in range(2)]
    stats = merged(merged(stats, rows), columns)
    top, total, moment, target_logit = stats
    lse = top + jnp.log(total)
    token_logprob = target_logit - lse
    entropy = lse - moment / total

    mean = sums[0, :prompt_count] / GROUP
    squares = sums[0, prompt_count : 2 * prompt_count]
    count = sums[0, 2 * prompt_count]
    spread = jnp.sqrt(jnp.maximum(squares / GROUP - mean * mean, 0.0))
    mean_roll = jnp.sum(member * mean[None, :], axis=1)
    spread_roll = jnp.sum(member * spread[None, :], axis=1)
    advantage = (scores - mean_roll) / jnp.maximum(spread_roll, 1.0)
    advantage = jnp.sum(jnp.where(own, advantage[:, None], 0.0), axis=0)
    ratio = jnp.exp(jnp.clip(token_logprob - old_logprob, -20.0, 20.0))
    surrogate = -jnp.minimum(ratio * advantage, jnp.clip(ratio, 0.8, 1.2) * advantage)
    shift = jnp.clip(ref_logprob - token_logprob, -20.0, 20.0)
    divergence = jnp.exp(shift) - shift - 1.0
    numer = jnp.sum(mask * (surrogate + 0.04 * divergence - 0.01 * entropy))
    numer = jnp.broadcast_to(numer, (1, LANES))
    numer = numer + over_dp(numer, 1)
    numer = numer + over_dp(numer, 3)
    loss = numer[0, 0] / count
    return (token_logprob, entropy, advantage, loss)


def solution(mesh):
    return jax.shard_map(
        per_device,
        mesh=mesh,
        in_specs=(
            P("dp", "vocab"),
            P(None, "vocab"),
            P("dp"),
            P("dp"),
            P("dp"),
            P("dp"),
            P("dp"),
            P("dp"),
        ),
        out_specs=(P("dp"), P("dp"), P("dp"), P()),
        check_vma=False,
    )
```

```python
import functools

import jax
import jax.numpy as jnp
from jax import lax
from jax.experimental import pallas as pl
from jax.experimental.pallas import tpu as pltpu
from jax.sharding import PartitionSpec as P

GROUP = 8
LANES = 128
SIDE = 4
STEPS = (0, -1, 1, 2)
F32 = jnp.float32


def device(y, x, core):
    return ((y % SIDE) * SIDE + x % SIDE) * 2 + core


def everyone():
    return [(v // (2 * SIDE), v // 2 % SIDE, v % 2) for v in range(2 * SIDE * SIDE)]


def send_on(value, phase, step):
    pairs = []
    for y, x, core in everyone():
        to = (y, x + step, core) if core == phase else (y + step, x, core)
        pairs.append((device(y, x, core), device(*to)))
    return lax.ppermute(value, "vocab", pairs)


def swap(value):
    pairs = [(device(y, x, core), device(y, x, 1 - core)) for y, x, core in everyone()]
    return lax.ppermute(value, "vocab", pairs)


def block_rows(second, partner, depth):
    v = lax.axis_index("vocab")
    core = (v & 1) ^ partner
    x, y = (v >> 1) & (SIDE - 1), v >> 3
    rows = []
    for first in STEPS:
        dx = jnp.where(core == 0, first, second)
        dy = jnp.where(core == 0, second, first)
        block = (((y + dy) & (SIDE - 1)) * SIDE + ((x + dx) & (SIDE - 1))) * 2 + core
        rows.append(pl.multiple_of(block * depth, 32))
    return rows


def column_tiles(width):
    return [(b, min(b + 512, width)) for b in range(0, width, 512)]


def fetches(parts, depth, there, here, sems):
    rows = [r for part in parts for r in block_rows(*part, depth)]
    return [
        pltpu.make_async_copy(there.at[pl.ds(r, depth)], here.at[pl.ds(r, depth)], sems.at[k])
        for k, r in enumerate(rows)
    ]


def load_kernel(parts, depth, there, here, sems):
    copies = fetches(parts, depth, there, here, sems)
    for c in copies:
        c.start()
    for c in copies:
        c.wait()


def multiply(blocks, parts, depth, w_ref, acc_in, acc, lhs):
    rows, at = [], 0
    for ref, part in zip(blocks, parts):
        size = ref.shape[0]
        lhs[:, at : at + size] = ref[...].T
        rows += block_rows(*part, depth)
        at += size
    for b, e in column_tiles(w_ref.shape[1]):
        w = jnp.concatenate([w_ref[pl.ds(r, depth), b:e] for r in rows], axis=0)
        out = jnp.dot(lhs[...], w, preferred_element_type=F32)
        acc[:, b:e] = out if acc_in is None else acc_in[:, b:e] + out


def step_kernel(parts, later, depth, *refs):
    blocks, rest = refs[: len(parts)], refs[len(parts) :]
    w_ref, there = rest[:2]
    acc_in = rest[2] if len(rest) == 7 else None
    acc, here, lhs, sems = rest[-4:]
    copies = fetches(later, depth, there, here, sems)
    for c in copies:
        c.start()
    multiply(blocks, parts, depth, w_ref, acc_in, acc, lhs)
    for c in copies:
        c.wait()


def last_kernel(parts, depth, *refs):
    w_ref, acc_in, target, stats, acc, lhs = refs[len(parts) :]
    multiply(refs[: len(parts)], parts, depth, w_ref, acc_in, acc, lhs)
    tok, width = acc.shape
    step = 64
    tops, totals, moments, picks = [], [], [], []
    lane = lax.broadcasted_iota(jnp.int32, (step, LANES), 1) + lax.axis_index("vocab") * width
    for r in range(0, tok, step):
        want = target[r : r + step, :] - lane
        top = acc[r : r + step, 0:LANES]
        pick = jnp.where(want == 0, top, 0.0)
        for b in range(LANES, width, LANES):
            piece = acc[r : r + step, b : b + LANES]
            top = jnp.maximum(top, piece)
            pick = jnp.where(want == b, piece, pick)
        total = jnp.zeros_like(top)
        moment = jnp.zeros_like(top)
        for b in range(0, width, LANES):
            piece = acc[r : r + step, b : b + LANES]
            scaled = jnp.exp(piece - top)
            total += scaled
            moment += scaled * piece
        tops.append(top)
        totals.append(total)
        moments.append(moment)
        picks.append(pick)
    top, total, moment, pick = (
        jnp.concatenate(p, axis=0).T for p in (tops, totals, moments, picks)
    )
    best = jnp.max(top, axis=0, keepdims=True)
    scale = jnp.exp(top - best)
    mine = jnp.concatenate(
        [
            best,
            jnp.sum(total * scale, axis=0, keepdims=True),
            jnp.sum(moment * scale, axis=0, keepdims=True),
            jnp.sum(pick, axis=0, keepdims=True),
        ],
        axis=0,
    )
    for k in range(stats.shape[0]):
        stats[k] = mine


def in_vmem(value):
    return pltpu.with_memory_space_constraint(value, pltpu.VMEM)


def vmem_specs(count):
    return [pl.BlockSpec(memory_space=pltpu.VMEM)] * count


def in_hbm(value):
    return pltpu.with_memory_space_constraint(value, pltpu.HBM)


HBM_SPEC = pl.BlockSpec(memory_space=pltpu.HBM)
LIMIT = 16 << 20


def cost(flops):
    return pl.CostEstimate(flops=flops, bytes_accessed=1 << 20, transcendentals=0)


def load(weight, parts, depth):
    return pl.pallas_call(
        functools.partial(load_kernel, parts, depth),
        out_shape=pltpu.VMEM(weight.shape, weight.dtype),
        in_specs=[HBM_SPEC],
        out_specs=pl.BlockSpec(memory_space=pltpu.VMEM),
        scratch_shapes=[pltpu.SemaphoreType.DMA((SIDE * len(parts),))],
        cost_estimate=cost(1 << 31),
        compiler_params=pltpu.CompilerParams(vmem_limit_bytes=LIMIT),
    )(in_hbm(weight))


def product(blocks, parts, later, held, weight, acc):
    depth_sum = sum(b.shape[0] for b in blocks)
    rows, width = blocks[0].shape[1], weight.shape[1]
    depth = weight.shape[0] // lax.axis_size("vocab")
    operands = [*blocks, held] + ([] if acc is None else [acc])
    operands = [in_vmem(o) for o in operands]
    operands.insert(len(blocks) + 1, in_hbm(weight))
    specs = vmem_specs(len(operands))
    specs[len(blocks) + 1] = HBM_SPEC
    aliases = {len(blocks): 1} | ({} if acc is None else {len(blocks) + 2: 0})
    return pl.pallas_call(
        functools.partial(step_kernel, parts, later, depth),
        out_shape=(
            jax.ShapeDtypeStruct((rows, width), F32),
            jax.ShapeDtypeStruct(weight.shape, weight.dtype),
        ),
        in_specs=specs,
        out_specs=tuple(vmem_specs(2)),
        scratch_shapes=[
            pltpu.VMEM((rows, depth_sum), jnp.bfloat16),
            pltpu.SemaphoreType.DMA((SIDE * len(later),)),
        ],
        input_output_aliases=aliases,
        cost_estimate=cost(2 * rows * depth_sum * width),
        compiler_params=pltpu.CompilerParams(vmem_limit_bytes=LIMIT),
    )(*operands)


def statistics(blocks, parts, held, acc, target):
    depth_sum = sum(b.shape[0] for b in blocks)
    rows, width = acc.shape
    size = lax.axis_size("vocab")
    operands = (*blocks, held, acc, target)
    return pl.pallas_call(
        functools.partial(last_kernel, parts, held.shape[0] // size),
        out_shape=jax.ShapeDtypeStruct((size, 4, rows), F32),
        in_specs=vmem_specs(len(operands)),
        out_specs=pl.BlockSpec(memory_space=pltpu.VMEM),
        scratch_shapes=[
            pltpu.VMEM((rows, width), F32),
            pltpu.VMEM((rows, depth_sum), jnp.bfloat16),
        ],
        cost_estimate=cost(2 * rows * depth_sum * width),
        compiler_params=pltpu.CompilerParams(vmem_limit_bytes=LIMIT),
    )(*[in_vmem(o) for o in operands])


def own_rolls(rolls, tokens):
    token = lax.broadcasted_iota(jnp.int32, (rolls, tokens), 1)
    roll = lax.broadcasted_iota(jnp.int32, (rolls, tokens), 0)
    return token // (tokens // rolls) == roll, token % (tokens // rolls)


def as_columns(columns, base=None):
    lane = lax.broadcasted_iota(jnp.int32, (columns[0].shape[0], LANES), 1)
    out = jnp.zeros(lane.shape, F32) if base is None else base
    for k, column in enumerate(columns):
        out = jnp.where(lane == k, column, out)
    return out


def token_kernel(lines, old, ref, live, info, token_logprob, entropy, pack):
    count = lines.shape[0]
    top = lines[0, 0:1, :]
    for k in range(1, count):
        top = jnp.maximum(top, lines[k, 0:1, :])
    total, moment, pick = (jnp.zeros_like(top) for _ in range(3))
    for k in range(count):
        scale = jnp.exp(lines[k, 0:1, :] - top)
        total += lines[k, 1:2, :] * scale
        moment += lines[k, 2:3, :] * scale
        pick += lines[k, 3:4, :]
    lse = top + jnp.log(total)
    logprob = pick - lse
    spread = lse - moment / total
    token_logprob[...] = logprob
    entropy[...] = spread
    ratio = jnp.exp(jnp.clip(logprob - old[...], -20.0, 20.0))
    held = jnp.clip(ratio, 0.8, 1.2)
    shift = jnp.clip(ref[...] - logprob, -20.0, 20.0)
    divergence = jnp.exp(shift) - shift - 1.0
    mask = live[...]

    def of_rolls(row):
        return jnp.sum(mask * row, axis=1, keepdims=True)

    sums = [of_rolls(jnp.minimum(ratio, held)), of_rolls(jnp.maximum(ratio, held))]
    sums += [of_rolls(0.04 * divergence - 0.01 * spread), jnp.sum(mask, axis=1, keepdims=True)]
    pack[...] = as_columns(sums, info[...])


def loss_kernel(prompts, *refs):
    packs, (advantage, loss) = refs[:-2], refs[-2:]
    rolls = packs[0].shape[0]
    every = jnp.concatenate([p[...] for p in packs], axis=0)
    low, high, extra, count, score, prompt = (every[:, k : k + 1] for k in range(6))
    gain = jnp.zeros_like(score)
    for g in range(prompts):
        here = prompt == g
        mean = jnp.sum(jnp.where(here, score, 0.0), axis=0, keepdims=True) / GROUP
        square = jnp.sum(jnp.where(here, score * score, 0.0), axis=0, keepdims=True)
        spread = jnp.sqrt(jnp.maximum(square / GROUP - mean * mean, 0.0))
        gain = jnp.where(here, (score - mean) / jnp.maximum(spread, 1.0), gain)
    terms = extra - gain * jnp.where(gain >= 0.0, low, high)
    loss[...] = jnp.sum(terms, axis=0, keepdims=True) / jnp.sum(count, axis=0, keepdims=True)
    own, _ = own_rolls(rolls, advantage.shape[1])
    advantage[...] = jnp.sum(jnp.where(own, gain[:rolls], 0.0), axis=0, keepdims=True)


def small(kernel, operands, shapes):
    return pl.pallas_call(
        kernel,
        out_shape=tuple(jax.ShapeDtypeStruct(s, F32) for s in shapes),
        in_specs=vmem_specs(len(operands)),
        out_specs=tuple(vmem_specs(len(shapes))),
        compiler_params=pltpu.CompilerParams(vmem_limit_bytes=LIMIT),
    )(*[in_vmem(o) for o in operands])


def per_device(hidden, weight, targets, old_logprob, ref_logprob, lengths, rewards, group_ids):
    tok_rows, depth = hidden.shape
    line = [hidden.T]
    for step in (1, -1, 2):
        line.append(send_on(line[0], 0, step))
    sets = (
        ((0, 0), (0, 1)),
        ((-1, 0), (1, 0)),
        ((-1, 1), (1, 1)),
        ((2, 0), (2, 1)),
    )
    held = load(weight, sets[0], depth)
    line = jnp.concatenate(line, axis=0)
    line_p = swap(line)
    far, far_p = [], []
    for step in (1, -1, 2):
        far.append(send_on(line, 1, step))
    acc, held = product((line, line_p), sets[0], sets[1], held, weight, None)
    for k in range(3):
        far_p.append(swap(far[k]))
    acc, held = product(far[:2], sets[1], sets[2], held, weight, acc)
    acc, held = product(far_p[:2], sets[2], sets[3], held, weight, acc)
    target = jnp.broadcast_to(targets[:, None], (tok_rows, LANES))
    lines = statistics((far[2], far_p[2]), sets[3], held, acc, target)
    lines = lax.all_to_all(lines, "vocab", 0, 0, tiled=True)
    rolls = rewards.shape[0]
    own, position = own_rolls(rolls, tok_rows)
    live = (own & (position < lengths[:, None])).astype(F32)
    blank = jnp.zeros((rolls, 1), F32)
    info = as_columns(
        [blank] * 4 + [rewards.astype(F32)[:, None], group_ids.astype(F32)[:, None]]
    )
    row = (1, tok_rows)
    token_logprob, entropy, pack = small(
        token_kernel,
        (lines, old_logprob[None], ref_logprob[None], live, info),
        (row, row, (rolls, LANES)),
    )
    size = lax.axis_size("dp")
    packs = [
        lax.ppermute(pack, "dp", [(v, (v + step) % size) for v in range(size)])
        for step in range(1, size)
    ]
    advantage, loss = small(
        functools.partial(loss_kernel, rolls * size // GROUP), (pack, *packs), (row, (1, 1))
    )
    return (token_logprob[0], entropy[0], advantage[0], loss[0, 0])


def solution(mesh):
    return jax.shard_map(
        per_device,
        mesh=mesh,
        in_specs=(
            P("dp", "vocab"),
            P(None, "vocab"),
            P("dp"),
            P("dp"),
            P("dp"),
            P("dp"),
            P("dp"),
            P("dp"),
        ),
        out_specs=(P("dp"), P("dp"), P("dp"), P()),
        check_vma=False,
    )
```

```python
import functools

import jax
import jax.numpy as jnp
from jax import lax
from jax.experimental import pallas as pl
from jax.experimental.pallas import tpu as pltpu
from jax.sharding import PartitionSpec as P

GROUP = 8
LANES = 128
SIDE = 4
STEPS = (0, -1, 1, 2)
F32 = jnp.float32


def device(y, x, core):
    return ((y % SIDE) * SIDE + x % SIDE) * 2 + core


def everyone():
    return [(v // (2 * SIDE), v // 2 % SIDE, v % 2) for v in range(2 * SIDE * SIDE)]


def send_on(value, phase, step):
    pairs = []
    for y, x, core in everyone():
        to = (y, x + step, core) if core == phase else (y + step, x, core)
        pairs.append((device(y, x, core), device(*to)))
    return lax.ppermute(value, "vocab", pairs)


def swap(value):
    pairs = [(device(y, x, core), device(y, x, 1 - core)) for y, x, core in everyone()]
    return lax.ppermute(value, "vocab", pairs)


def block_rows(blocks, partner, depth):
    v = lax.axis_index("vocab")
    core = (v & 1) ^ partner
    x, y = (v >> 1) & (SIDE - 1), v >> 3
    rows = []
    for first, second in blocks:
        dx = jnp.where(core == 0, first, second)
        dy = jnp.where(core == 0, second, first)
        block = (((y + dy) & (SIDE - 1)) * SIDE + ((x + dx) & (SIDE - 1))) * 2 + core
        rows.append(pl.multiple_of(block * depth, 32))
    return rows


LINE = tuple((first, 0) for first in STEPS)
SIDES = ((0, -1), (0, 1))


def far_blocks(second, steps=STEPS):
    return tuple((first, second) for first in steps)


def padded(size):
    return -(-size // 256) * 256


def column_tiles(width):
    return [(b, min(b + 512, width)) for b in range(0, width, 512)]


def fetches(parts, depth, there, here, sems):
    rows = [r for part in parts for r in block_rows(*part, depth)]
    return [
        pltpu.make_async_copy(there.at[pl.ds(r, depth)], here.at[pl.ds(r, depth)], sems.at[k])
        for k, r in enumerate(rows)
    ]


def load_kernel(parts, depth, there, here, sems):
    copies = fetches(parts, depth, there, here, sems)
    for c in copies:
        c.start()
    for c in copies:
        c.wait()


def rows_between(refs, lo, hi):
    pieces, at = [], 0
    for ref in refs:
        size = ref.shape[0]
        b, e = max(lo - at, 0), min(hi - at, size)
        if b < e:
            pieces.append(ref[b:e, :])
        at += size
    if at < hi:
        pieces.append(jnp.zeros((hi - max(lo, at), refs[0].shape[1]), refs[0].dtype))
    return jnp.concatenate(pieces, axis=0) if len(pieces) > 1 else pieces[0]


def multiply(blocks, parts, depth, w_ref, lhs, emit):
    rows = [r for part in parts for r in block_rows(*part, depth)]
    extra = lhs.shape[1] - len(rows) * depth
    for k in range(0, lhs.shape[1], 256):
        lhs[:, k : k + 256] = rows_between(blocks, k, k + 256).T
    for b, e in column_tiles(w_ref.shape[1]):
        w = [w_ref[pl.ds(r, depth), b:e] for r in rows]
        if extra:
            w.append(w_ref[pl.ds(rows[0], extra), b:e])
        emit(b, e, jnp.dot(lhs[...], jnp.concatenate(w, axis=0), preferred_element_type=F32))


def step_kernel(parts, later, depth, *refs):
    blocks, rest = refs[: len(parts)], refs[len(parts) :]
    w_ref, there = rest[:2]
    acc_in = rest[2] if len(rest) == 7 else None
    acc, here, lhs, sems = rest[-4:]
    copies = fetches(later, depth, there, here, sems)
    for c in copies:
        c.start()

    def emit(b, e, out):
        acc[:, b:e] = out if acc_in is None else acc_in[:, b:e] + out

    multiply(blocks, parts, depth, w_ref, lhs, emit)
    for c in copies:
        c.wait()


def last_kernel(parts, depth, *refs):
    w_ref, acc_in, target, stats, acc, tops, picks, lhs = refs[len(parts) :]
    tok, width = acc.shape
    step = 64
    first = lax.axis_index("vocab") * width
    lane = lax.broadcasted_iota(jnp.int32, (tok, LANES), 1) + first

    def emit(b, e, out):
        new = acc_in[:, b:e] + out
        acc[:, b:e] = new
        pieces = [new[:, k : k + LANES] for k in range(0, e - b, LANES)]
        top = functools.reduce(jnp.maximum, pieces)
        want = target[...] - lane
        pick = jnp.zeros_like(top) if b == 0 else picks[...]
        for k, piece in enumerate(pieces):
            pick = jnp.where(want == b + k * LANES, piece, pick)
        tops[...] = top if b == 0 else jnp.maximum(tops[...], top)
        picks[...] = pick

    multiply(refs[: len(parts)], parts, depth, w_ref, lhs, emit)
    totals, moments = [], []
    for r in range(0, tok, step):
        top = tops[r : r + step, :]
        total = jnp.zeros_like(top)
        moment = jnp.zeros_like(top)
        for b in range(0, width, LANES):
            piece = acc[r : r + step, b : b + LANES]
            scaled = jnp.exp(piece - top)
            total += scaled
            moment += scaled * piece
        totals.append(total)
        moments.append(moment)
    total, moment = (jnp.concatenate(p, axis=0).T for p in (totals, moments))
    top, pick = tops[...].T, picks[...].T
    best = jnp.max(top, axis=0, keepdims=True)
    scale = jnp.exp(top - best)
    mine = jnp.concatenate(
        [
            best,
            jnp.sum(total * scale, axis=0, keepdims=True),
            jnp.sum(moment * scale, axis=0, keepdims=True),
            jnp.sum(pick, axis=0, keepdims=True),
        ],
        axis=0,
    )
    for k in range(stats.shape[0]):
        stats[k] = mine


def in_vmem(value):
    return pltpu.with_memory_space_constraint(value, pltpu.VMEM)


def vmem_specs(count):
    return [pl.BlockSpec(memory_space=pltpu.VMEM)] * count


def in_hbm(value):
    return pltpu.with_memory_space_constraint(value, pltpu.HBM)


HBM_SPEC = pl.BlockSpec(memory_space=pltpu.HBM)
LIMIT = 16 << 20


def cost(flops):
    return pl.CostEstimate(flops=flops, bytes_accessed=1 << 20, transcendentals=0)


def count_of(parts):
    return sum(len(blocks) for blocks, _ in parts)


def load(weight, parts, depth):
    return pl.pallas_call(
        functools.partial(load_kernel, parts, depth),
        out_shape=pltpu.VMEM(weight.shape, weight.dtype),
        in_specs=[HBM_SPEC],
        out_specs=pl.BlockSpec(memory_space=pltpu.VMEM),
        scratch_shapes=[pltpu.SemaphoreType.DMA((count_of(parts),))],
        cost_estimate=cost(1 << 31),
        compiler_params=pltpu.CompilerParams(vmem_limit_bytes=LIMIT),
    )(in_hbm(weight))


def product(blocks, parts, later, held, weight, acc):
    depth_sum = sum(b.shape[0] for b in blocks)
    rows, width = blocks[0].shape[1], weight.shape[1]
    depth = weight.shape[0] // lax.axis_size("vocab")
    operands = [*blocks, held] + ([] if acc is None else [acc])
    operands = [in_vmem(o) for o in operands]
    operands.insert(len(blocks) + 1, in_hbm(weight))
    specs = vmem_specs(len(operands))
    specs[len(blocks) + 1] = HBM_SPEC
    aliases = {len(blocks): 1} | ({} if acc is None else {len(blocks) + 2: 0})
    return pl.pallas_call(
        functools.partial(step_kernel, parts, later, depth),
        out_shape=(
            jax.ShapeDtypeStruct((rows, width), F32),
            jax.ShapeDtypeStruct(weight.shape, weight.dtype),
        ),
        in_specs=specs,
        out_specs=tuple(vmem_specs(2)),
        scratch_shapes=[
            pltpu.VMEM((rows, padded(depth_sum)), jnp.bfloat16),
            pltpu.SemaphoreType.DMA((count_of(later),)),
        ],
        input_output_aliases=aliases,
        cost_estimate=cost(2 * rows * depth_sum * width),
        compiler_params=pltpu.CompilerParams(vmem_limit_bytes=LIMIT),
    )(*operands)


def statistics(blocks, parts, held, acc, target):
    depth_sum = sum(b.shape[0] for b in blocks)
    rows, width = acc.shape
    size = lax.axis_size("vocab")
    operands = (*blocks, held, acc, target)
    return pl.pallas_call(
        functools.partial(last_kernel, parts, held.shape[0] // size),
        out_shape=jax.ShapeDtypeStruct((size, 4, rows), F32),
        in_specs=vmem_specs(len(operands)),
        out_specs=pl.BlockSpec(memory_space=pltpu.VMEM),
        scratch_shapes=[
            pltpu.VMEM((rows, width), F32),
            pltpu.VMEM((rows, LANES), F32),
            pltpu.VMEM((rows, LANES), F32),
            pltpu.VMEM((rows, padded(depth_sum)), jnp.bfloat16),
        ],
        cost_estimate=cost(2 * rows * depth_sum * width),
        compiler_params=pltpu.CompilerParams(vmem_limit_bytes=LIMIT),
    )(*[in_vmem(o) for o in operands])


def own_rolls(rolls, tokens):
    token = lax.broadcasted_iota(jnp.int32, (rolls, tokens), 1)
    roll = lax.broadcasted_iota(jnp.int32, (rolls, tokens), 0)
    return token // (tokens // rolls) == roll, token % (tokens // rolls)


def as_columns(columns, base=None):
    lane = lax.broadcasted_iota(jnp.int32, (columns[0].shape[0], LANES), 1)
    out = jnp.zeros(lane.shape, F32) if base is None else base
    for k, column in enumerate(columns):
        out = jnp.where(lane == k, column, out)
    return out


def token_kernel(lines, old, ref, live, info, token_logprob, entropy, pack):
    count = lines.shape[0]
    top = lines[0, 0:1, :]
    for k in range(1, count):
        top = jnp.maximum(top, lines[k, 0:1, :])
    total, moment, pick = (jnp.zeros_like(top) for _ in range(3))
    for k in range(count):
        scale = jnp.exp(lines[k, 0:1, :] - top)
        total += lines[k, 1:2, :] * scale
        moment += lines[k, 2:3, :] * scale
        pick += lines[k, 3:4, :]
    lse = top + jnp.log(total)
    logprob = pick - lse
    spread = lse - moment / total
    token_logprob[...] = logprob
    entropy[...] = spread
    ratio = jnp.exp(jnp.clip(logprob - old[...], -20.0, 20.0))
    held = jnp.clip(ratio, 0.8, 1.2)
    shift = jnp.clip(ref[...] - logprob, -20.0, 20.0)
    divergence = jnp.exp(shift) - shift - 1.0
    mask = live[...]

    def of_rolls(row):
        return jnp.sum(mask * row, axis=1, keepdims=True)

    sums = [of_rolls(jnp.minimum(ratio, held)), of_rolls(jnp.maximum(ratio, held))]
    sums += [of_rolls(0.04 * divergence - 0.01 * spread), jnp.sum(mask, axis=1, keepdims=True)]
    pack[...] = as_columns(sums, info[...])


def loss_kernel(prompts, rolls, pack, advantage, loss):
    every = pack[...]
    low, high, extra, count, score, prompt = (every[:, k : k + 1] for k in range(6))
    gain = jnp.zeros_like(score)
    for g in range(prompts):
        here = prompt == g
        mean = jnp.sum(jnp.where(here, score, 0.0), axis=0, keepdims=True) / GROUP
        square = jnp.sum(jnp.where(here, score * score, 0.0), axis=0, keepdims=True)
        spread = jnp.sqrt(jnp.maximum(square / GROUP - mean * mean, 0.0))
        gain = jnp.where(here, (score - mean) / jnp.maximum(spread, 1.0), gain)
    terms = extra - gain * jnp.where(gain >= 0.0, low, high)
    loss[...] = jnp.sum(terms, axis=0, keepdims=True) / jnp.sum(count, axis=0, keepdims=True)
    own, _ = own_rolls(rolls, advantage.shape[1])
    advantage[...] = jnp.sum(jnp.where(own, gain[:rolls], 0.0), axis=0, keepdims=True)


def small(kernel, operands, shapes):
    return pl.pallas_call(
        kernel,
        out_shape=tuple(jax.ShapeDtypeStruct(s, F32) for s in shapes),
        in_specs=vmem_specs(len(operands)),
        out_specs=tuple(vmem_specs(len(shapes))),
        compiler_params=pltpu.CompilerParams(vmem_limit_bytes=LIMIT),
    )(*[in_vmem(o) for o in operands])


def per_device(hidden, weight, targets, old_logprob, ref_logprob, lengths, rewards, group_ids):
    tok_rows, depth = hidden.shape
    mine = hidden.T
    line = [mine]
    for step in (1, -1, 2):
        line.append(send_on(mine, 0, step))
    sides = []
    for step in (1, -1):
        sides.append(send_on(mine, 1, step))
    others = STEPS[1:]
    sets = (
        ((LINE, 0), (LINE, 1)),
        ((SIDES, 0), (SIDES, 1)),
        ((far_blocks(2), 0),),
        ((far_blocks(2), 1),),
        ((far_blocks(-1, others), 0), (far_blocks(1, others), 0)),
        ((far_blocks(-1, others), 1), (far_blocks(1, others), 1)),
    )
    held = load(weight, sets[0], depth)
    line = jnp.concatenate(line, axis=0)
    far, far_p = {}, {}
    for step in (2, 1, -1):
        far[step] = send_on(line if step == 2 else line[depth:], 1, step)
    line_p = swap(line)
    sides = jnp.concatenate(sides, axis=0)
    sides_p = swap(sides)
    acc, held = product((line, line_p), sets[0], sets[1], held, weight, None)
    acc, held = product((sides, sides_p), sets[1], sets[2], held, weight, acc)
    for step in (2, 1, -1):
        far_p[step] = swap(far[step])
    acc, held = product((far[2],), sets[2], sets[3], held, weight, acc)
    acc, held = product((far_p[2],), sets[3], sets[4], held, weight, acc)
    acc, held = product((far[1], far[-1]), sets[4], sets[5], held, weight, acc)
    target = jnp.broadcast_to(targets[:, None], (tok_rows, LANES))
    lines = statistics((far_p[1], far_p[-1]), sets[5], held, acc, target)
    lines = lax.all_to_all(lines, "vocab", 0, 0, tiled=True)
    rolls = rewards.shape[0]
    own, position = own_rolls(rolls, tok_rows)
    live = (own & (position < lengths[:, None])).astype(F32)
    blank = jnp.zeros((rolls, 1), F32)
    info = as_columns([blank] * 4 + [rewards.astype(F32)[:, None], group_ids.astype(F32)[:, None]])
    row = (1, tok_rows)
    token_logprob, entropy, pack = small(
        token_kernel,
        (lines, old_logprob[None], ref_logprob[None], live, info),
        (row, row, (rolls, LANES)),
    )
    for mask in (1, 3):
        pairs = [(v, v ^ mask) for v in range(lax.axis_size("dp"))]
        pack = jnp.concatenate([pack, lax.ppermute(pack, "dp", pairs)], axis=0)
    prompts = rolls * lax.axis_size("dp") // GROUP
    advantage, loss = small(
        functools.partial(loss_kernel, prompts, rolls), (pack,), (row, (1, 1))
    )
    return (token_logprob[0], entropy[0], advantage[0], loss[0, 0])


def solution(mesh):
    return jax.shard_map(
        per_device,
        mesh=mesh,
        in_specs=(
            P("dp", "vocab"),
            P(None, "vocab"),
            P("dp"),
            P("dp"),
            P("dp"),
            P("dp"),
            P("dp"),
            P("dp"),
        ),
        out_specs=(P("dp"), P("dp"), P("dp"), P()),
        check_vma=False,
    )
```

```python
import functools

import jax
import jax.numpy as jnp
from jax import lax
from jax.experimental import pallas as pl
from jax.experimental.pallas import tpu as pltpu
from jax.sharding import PartitionSpec as P

GROUP = 8
LANES = 128
SIDE = 4
STEPS = (0, -1, 1, 2)
F32 = jnp.float32


def device(y, x, core):
    return ((y % SIDE) * SIDE + x % SIDE) * 2 + core


def everyone():
    return [(v // (2 * SIDE), v // 2 % SIDE, v % 2) for v in range(2 * SIDE * SIDE)]


def send_on(value, phase, step):
    pairs = []
    for y, x, core in everyone():
        to = (y, x + step, core) if core == phase else (y + step, x, core)
        pairs.append((device(y, x, core), device(*to)))
    return lax.ppermute(value, "vocab", pairs)


def swap(value):
    pairs = [(device(y, x, core), device(y, x, 1 - core)) for y, x, core in everyone()]
    return lax.ppermute(value, "vocab", pairs)


def block_rows(blocks, partner, depth):
    v = lax.axis_index("vocab")
    core = (v & 1) ^ partner
    x, y = (v >> 1) & (SIDE - 1), v >> 3
    rows = []
    for first, second in blocks:
        dx = jnp.where(core == 0, first, second)
        dy = jnp.where(core == 0, second, first)
        block = (((y + dy) & (SIDE - 1)) * SIDE + ((x + dx) & (SIDE - 1))) * 2 + core
        rows.append(pl.multiple_of(block * depth, 32))
    return rows


LINE = tuple((first, 0) for first in STEPS)
SIDES = ((0, -1), (0, 1))


def far_blocks(second, steps=STEPS):
    return tuple((first, second) for first in steps)


def padded(size):
    return -(-size // 256) * 256


def column_tiles(width):
    return [(b, min(b + 512, width)) for b in range(0, width, 512)]


def fetches(parts, depth, there, here, sems):
    rows = [r for part in parts for r in block_rows(*part, depth)]
    return [
        pltpu.make_async_copy(there.at[pl.ds(r, depth)], here.at[pl.ds(r, depth)], sems.at[k])
        for k, r in enumerate(rows)
    ]


def load_kernel(parts, depth, there, here, sems):
    copies = fetches(parts, depth, there, here, sems)
    for c in copies:
        c.start()
    for c in copies:
        c.wait()


def rows_between(refs, lo, hi):
    pieces, at = [], 0
    for ref in refs:
        size = ref.shape[0]
        b, e = max(lo - at, 0), min(hi - at, size)
        if b < e:
            pieces.append(ref[b:e, :])
        at += size
    if at < hi:
        pieces.append(jnp.zeros((hi - max(lo, at), refs[0].shape[1]), refs[0].dtype))
    return jnp.concatenate(pieces, axis=0) if len(pieces) > 1 else pieces[0]


def multiply(blocks, parts, depth, w_ref, lhs, emit):
    rows = [r for part in parts for r in block_rows(*part, depth)]
    extra = lhs.shape[1] - len(rows) * depth
    for k in range(0, lhs.shape[1], 256):
        lhs[:, k : k + 256] = rows_between(blocks, k, k + 256).T
    for b, e in column_tiles(w_ref.shape[1]):
        w = [w_ref[pl.ds(r, depth), b:e] for r in rows]
        if extra:
            w.append(w_ref[pl.ds(rows[0], extra), b:e])
        emit(b, e, jnp.dot(lhs[...], jnp.concatenate(w, axis=0), preferred_element_type=F32))


def step_kernel(parts, later, depth, *refs):
    blocks, rest = refs[: len(parts)], refs[len(parts) :]
    w_ref, there = rest[:2]
    acc_in = rest[2] if len(rest) == 7 else None
    acc, here, lhs, sems = rest[-4:]
    copies = fetches(later, depth, there, here, sems)
    for c in copies:
        c.start()

    def emit(b, e, out):
        acc[:, b:e] = out if acc_in is None else acc_in[:, b:e] + out

    multiply(blocks, parts, depth, w_ref, lhs, emit)
    for c in copies:
        c.wait()


def last_kernel(parts, depth, *refs):
    w_ref, acc_in, target, stats, tops, totals, moments, picks, lhs = refs[len(parts) :]
    tok = acc_in.shape[0]
    step = 64
    first = lax.axis_index("vocab") * w_ref.shape[1]
    lane = lax.broadcasted_iota(jnp.int32, (step, LANES), 1) + first

    def emit(b, e, out):
        for r in range(0, tok, step):
            at = slice(r, r + step)
            pieces = [
                acc_in[at, k : k + LANES] + out[at, k - b : k - b + LANES]
                for k in range(b, e, LANES)
            ]
            top = functools.reduce(jnp.maximum, pieces)
            if b == 0:
                total = moment = pick = jnp.zeros_like(top)
            else:
                before = tops[at, :]
                top = jnp.maximum(before, top)
                scale = jnp.exp(before - top)
                total, moment = totals[at, :] * scale, moments[at, :] * scale
                pick = picks[at, :]
            want = target[at, :] - lane
            for k, piece in enumerate(pieces):
                scaled = jnp.exp(piece - top)
                total += scaled
                moment += scaled * piece
                pick = jnp.where(want == b + k * LANES, piece, pick)
            tops[at, :] = top
            totals[at, :] = total
            moments[at, :] = moment
            picks[at, :] = pick

    multiply(refs[: len(parts)], parts, depth, w_ref, lhs, emit)
    top, total, moment, pick = (ref[...].T for ref in (tops, totals, moments, picks))
    best = jnp.max(top, axis=0, keepdims=True)
    scale = jnp.exp(top - best)
    total = jnp.sum(total * scale, axis=0, keepdims=True)
    moment = jnp.sum(moment * scale, axis=0, keepdims=True)
    pick = jnp.sum(pick, axis=0, keepdims=True)
    mine = jnp.concatenate([best + jnp.log(total), moment / total, pick], axis=1)
    for k in range(stats.shape[0]):
        stats[k] = mine


def in_vmem(value):
    return pltpu.with_memory_space_constraint(value, pltpu.VMEM)


def vmem_specs(count):
    return [pl.BlockSpec(memory_space=pltpu.VMEM)] * count


def in_hbm(value):
    return pltpu.with_memory_space_constraint(value, pltpu.HBM)


HBM_SPEC = pl.BlockSpec(memory_space=pltpu.HBM)
LIMIT = 16 << 20


def cost(flops):
    return pl.CostEstimate(flops=flops, bytes_accessed=1 << 20, transcendentals=0)


def count_of(parts):
    return sum(len(blocks) for blocks, _ in parts)


def load(weight, parts, depth):
    return pl.pallas_call(
        functools.partial(load_kernel, parts, depth),
        out_shape=pltpu.VMEM(weight.shape, weight.dtype),
        in_specs=[HBM_SPEC],
        out_specs=pl.BlockSpec(memory_space=pltpu.VMEM),
        scratch_shapes=[pltpu.SemaphoreType.DMA((count_of(parts),))],
        cost_estimate=cost(1 << 31),
        compiler_params=pltpu.CompilerParams(vmem_limit_bytes=LIMIT),
    )(in_hbm(weight))


def product(blocks, parts, later, held, weight, acc):
    depth_sum = sum(b.shape[0] for b in blocks)
    rows, width = blocks[0].shape[1], weight.shape[1]
    depth = weight.shape[0] // lax.axis_size("vocab")
    operands = [*blocks, held] + ([] if acc is None else [acc])
    operands = [in_vmem(o) for o in operands]
    operands.insert(len(blocks) + 1, in_hbm(weight))
    specs = vmem_specs(len(operands))
    specs[len(blocks) + 1] = HBM_SPEC
    aliases = {len(blocks): 1} | ({} if acc is None else {len(blocks) + 2: 0})
    return pl.pallas_call(
        functools.partial(step_kernel, parts, later, depth),
        out_shape=(
            jax.ShapeDtypeStruct((rows, width), F32),
            jax.ShapeDtypeStruct(weight.shape, weight.dtype),
        ),
        in_specs=specs,
        out_specs=tuple(vmem_specs(2)),
        scratch_shapes=[
            pltpu.VMEM((rows, padded(depth_sum)), jnp.bfloat16),
            pltpu.SemaphoreType.DMA((count_of(later),)),
        ],
        input_output_aliases=aliases,
        cost_estimate=cost(2 * rows * depth_sum * width),
        compiler_params=pltpu.CompilerParams(vmem_limit_bytes=LIMIT),
    )(*operands)


def statistics(blocks, parts, held, acc, target):
    depth_sum = sum(b.shape[0] for b in blocks)
    rows, width = acc.shape
    size = lax.axis_size("vocab")
    operands = (*blocks, held, acc, target)
    return pl.pallas_call(
        functools.partial(last_kernel, parts, held.shape[0] // size),
        out_shape=jax.ShapeDtypeStruct((size, 1, 3 * rows), F32),
        in_specs=vmem_specs(len(operands)),
        out_specs=pl.BlockSpec(memory_space=pltpu.VMEM),
        scratch_shapes=[
            *[pltpu.VMEM((rows, LANES), F32)] * 4,
            pltpu.VMEM((rows, padded(depth_sum)), jnp.bfloat16),
        ],
        cost_estimate=cost(2 * rows * depth_sum * width),
        compiler_params=pltpu.CompilerParams(vmem_limit_bytes=LIMIT),
    )(*[in_vmem(o) for o in operands])


def own_rolls(rolls, tokens):
    token = lax.broadcasted_iota(jnp.int32, (rolls, tokens), 1)
    roll = lax.broadcasted_iota(jnp.int32, (rolls, tokens), 0)
    return token // (tokens // rolls) == roll, token % (tokens // rolls)


def as_columns(columns, base=None):
    lane = lax.broadcasted_iota(jnp.int32, (columns[0].shape[0], LANES), 1)
    out = jnp.zeros(lane.shape, F32) if base is None else base
    for k, column in enumerate(columns):
        out = jnp.where(lane == k, column, out)
    return out


def token_kernel(lines, old, ref, live, info, token_logprob, entropy, pack):
    count, tok = lines.shape[0], old.shape[1]

    def line(k, what):
        return lines[k, 0:1, what * tok : (what + 1) * tok]

    top = line(0, 0)
    for k in range(1, count):
        top = jnp.maximum(top, line(k, 0))
    total, moment, pick = (jnp.zeros_like(top) for _ in range(3))
    for k in range(count):
        scale = jnp.exp(line(k, 0) - top)
        total += scale
        moment += line(k, 1) * scale
        pick += line(k, 2)
    lse = top + jnp.log(total)
    logprob = pick - lse
    spread = lse - moment / total
    token_logprob[...] = logprob
    entropy[...] = spread
    ratio = jnp.exp(jnp.clip(logprob - old[...], -20.0, 20.0))
    held = jnp.clip(ratio, 0.8, 1.2)
    shift = jnp.clip(ref[...] - logprob, -20.0, 20.0)
    divergence = jnp.exp(shift) - shift - 1.0
    mask = live[...]

    def of_rolls(row):
        return jnp.sum(mask * row, axis=1, keepdims=True)

    sums = [of_rolls(jnp.minimum(ratio, held)), of_rolls(jnp.maximum(ratio, held))]
    sums += [of_rolls(0.04 * divergence - 0.01 * spread), jnp.sum(mask, axis=1, keepdims=True)]
    pack[...] = as_columns(sums, info[...])


def loss_kernel(prompts, rolls, pack, advantage, loss):
    every = pack[...]
    low, high, extra, count, score, prompt = (every[:, k : k + 1] for k in range(6))
    gain = jnp.zeros_like(score)
    for g in range(prompts):
        here = prompt == g
        mean = jnp.sum(jnp.where(here, score, 0.0), axis=0, keepdims=True) / GROUP
        square = jnp.sum(jnp.where(here, score * score, 0.0), axis=0, keepdims=True)
        spread = jnp.sqrt(jnp.maximum(square / GROUP - mean * mean, 0.0))
        gain = jnp.where(here, (score - mean) / jnp.maximum(spread, 1.0), gain)
    terms = extra - gain * jnp.where(gain >= 0.0, low, high)
    loss[...] = jnp.sum(terms, axis=0, keepdims=True) / jnp.sum(count, axis=0, keepdims=True)
    own, _ = own_rolls(rolls, advantage.shape[1])
    advantage[...] = jnp.sum(jnp.where(own, gain[:rolls], 0.0), axis=0, keepdims=True)


def small(kernel, operands, shapes):
    return pl.pallas_call(
        kernel,
        out_shape=tuple(jax.ShapeDtypeStruct(s, F32) for s in shapes),
        in_specs=vmem_specs(len(operands)),
        out_specs=tuple(vmem_specs(len(shapes))),
        compiler_params=pltpu.CompilerParams(vmem_limit_bytes=LIMIT),
    )(*[in_vmem(o) for o in operands])


def per_device(hidden, weight, targets, old_logprob, ref_logprob, lengths, rewards, group_ids):
    tok_rows, depth = hidden.shape
    mine = hidden.T
    line = [mine]
    for step in (1, -1, 2):
        line.append(send_on(mine, 0, step))
    sides = []
    for step in (1, -1):
        sides.append(send_on(mine, 1, step))
    others = STEPS[1:]
    sets = (
        ((LINE, 0), (LINE, 1)),
        ((SIDES, 0), (SIDES, 1)),
        ((far_blocks(2), 0),),
        ((far_blocks(2), 1),),
        ((far_blocks(-1, others), 0), (far_blocks(1, others), 0)),
        ((far_blocks(-1, others), 1), (far_blocks(1, others), 1)),
    )
    held = load(weight, sets[0], depth)
    line = jnp.concatenate(line, axis=0)
    far, far_p = {}, {}
    for step in (2, 1, -1):
        far[step] = send_on(line if step == 2 else line[depth:], 1, step)
    line_p = swap(line)
    sides = jnp.concatenate(sides, axis=0)
    sides_p = swap(sides)
    acc, held = product((line, line_p), sets[0], sets[1], held, weight, None)
    acc, held = product((sides, sides_p), sets[1], sets[2], held, weight, acc)
    for step in (2, 1, -1):
        far_p[step] = swap(far[step])
    acc, held = product((far[2],), sets[2], sets[3], held, weight, acc)
    acc, held = product((far_p[2],), sets[3], sets[4], held, weight, acc)
    acc, held = product((far[1], far[-1]), sets[4], sets[5], held, weight, acc)
    target = jnp.broadcast_to(targets[:, None], (tok_rows, LANES))
    lines = statistics((far_p[1], far_p[-1]), sets[5], held, acc, target)
    lines = lax.all_to_all(lines, "vocab", 0, 0, tiled=True)
    rolls = rewards.shape[0]
    own, position = own_rolls(rolls, tok_rows)
    live = (own & (position < lengths[:, None])).astype(F32)
    blank = jnp.zeros((rolls, 1), F32)
    info = as_columns([blank] * 4 + [rewards.astype(F32)[:, None], group_ids.astype(F32)[:, None]])
    row = (1, tok_rows)
    token_logprob, entropy, pack = small(
        token_kernel,
        (lines, old_logprob[None], ref_logprob[None], live, info),
        (row, row, (rolls, LANES)),
    )
    for mask in (1, 3):
        pairs = [(v, v ^ mask) for v in range(lax.axis_size("dp"))]
        pack = jnp.concatenate([pack, lax.ppermute(pack, "dp", pairs)], axis=0)
    prompts = rolls * lax.axis_size("dp") // GROUP
    advantage, loss = small(
        functools.partial(loss_kernel, prompts, rolls), (pack,), (row, (1, 1))
    )
    return (token_logprob[0], entropy[0], advantage[0], loss[0, 0])


def solution(mesh):
    return jax.shard_map(
        per_device,
        mesh=mesh,
        in_specs=(
            P("dp", "vocab"),
            P(None, "vocab"),
            P("dp"),
            P("dp"),
            P("dp"),
            P("dp"),
            P("dp"),
            P("dp"),
        ),
        out_specs=(P("dp"), P("dp"), P("dp"), P()),
        check_vma=False,
    )
```
